32 devices in a mesh: expert: 4 (over x, core), dp: 8 (over z, y).
Axes of the slice: x: 2, y: 2, z: 4, core: 2. Of those that a mesh axis runs over, the one named last changes fastest.
Arguments:
- cotangents: bfloat16 [4096, 2048], P(('expert', 'dp')), may hold values from -0.59765625 to 0.59765625
- routes: int32 [4096, 2], P(('expert', 'dp')), may hold values from 0 to 3, all different within a row; in each aligned block of 128 rows (0 to 127, 128 to 255, ...) at most 80 rows name the same one
- gate_probs: float32 [4096, 2], P(('expert', 'dp')), may hold values from 0.1 to 0.9
- hidden_now: bfloat16 [4, 8, 4, 80, 7168], P('expert', 'dp'), may hold values from -6 to 6
- hidden_prev: bfloat16 [4, 8, 4, 80, 7168], P('expert', 'dp'), may hold values from -6 to 6
- cotan_prev: bfloat16 [4, 8, 320, 2048], P('expert', 'dp'), may hold values from -0.29882812 to 0.29882812
- trigger: int32 [4, 8, 56], P('expert', 'dp'), may hold values from 0 to 1, as said below
- stale_sum: float32 [4, 7168, 2048], P('expert', None, 'dp'), may hold values from -12 to 12
Outputs:
- new_sum: float32 [4, 7168, 2048], P('expert', None, 'dp')
- margins: float32 [4, 8, 56], P('expert', 'dp')
The draws below stay inside these ranges and needn't reach their ends.
Inputs may be any that keep to these rules, and one draw needn't show every extreme that they name: `routes`: in the rows of one device each expert is named at most 80 times. `trigger`: each worker's row of 56 entries holds between 1 and 16 ones, and some worker's row holds exactly 16.
All inputs are finite; a program needn't handle non-finite values.
Results may differ from the reference program's by a relative error of at most 0.0055.
Values may be sent and summed in bfloat16 or wider, within the bound.
A program may use at most 192 MiB of HBM per device.

```python
import math
import jax
import jax.numpy as jnp
import numpy as np
from jax import lax

TOK_DEV = 128
DW = 2048
FFW = 7168
BLOCK = 128
TRIG = 16
EXPERTS = 4
CAP = 80
BLOCKS = 56
TOKENS = 4096
N_DP = 8


def draw_trigger(key, part):
    workers = EXPERTS * N_DP
    count_key, pick_key, order_key = jax.random.split(key, 3)
    counts = jax.random.randint(count_key, (workers,), 1, TRIG + 1)
    busiest = jax.random.randint(pick_key, (), 0, workers)
    counts = jnp.where(jnp.arange(workers) == busiest, TRIG, counts)
    orders = jax.vmap(lambda one_key: jax.random.permutation(one_key, BLOCKS))(jax.random.split(order_key, workers))
    block_ranks = jnp.argsort(orders, axis=1)
    return (block_ranks < counts[:, None]).astype(jnp.int32).reshape(EXPERTS, N_DP, BLOCKS)


def block_scale(stream_key, dims, shards, smallest, largest):
    def one(dim, parts):
        draws = jax.random.uniform(jax.random.fold_in(jax.random.fold_in(stream_key, 6), dim), (parts,), jnp.float32, smallest / len(shards), largest / len(shards))
        return jnp.repeat(jnp.exp(draws), dims[dim] // parts).reshape((-1,) + (1,) * (len(dims) - dim - 1))

    factor_of = one(*shards[0])
    for cut in shards[1:]:
        factor_of = factor_of * one(*cut)
    return factor_of


def assign_block(own_key, own, number, rows, count, top, most, slope):
    ranking = jax.random.permutation(own_key, count)
    crowded, usual = shares(count, rows * top, most, slope, True), shares(count, rows * top, most, slope, False)
    places = jnp.arange(count)

    def named(tallies, offset_by):
        used = int((tallies > 0).sum())
        fixed = max(1, used // 4)
        moved = fixed + (places - fixed + offset_by * (used - fixed)) % max(1, count - fixed)
        return jnp.zeros((count,), jnp.int32).at[ranking[jnp.where(places < fixed, places, moved)]].set(jnp.asarray(tallies, jnp.int32))

    tallies = jnp.where(number % 4 == 0, named(crowded, number // 4), named(usual, number - number // 4 - 1))
    mixed = jax.random.permutation(jax.random.fold_in(own, 3), count)
    source_of, sink = mixed[0:count // 2 * 2:2], mixed[1:count // 2 * 2:2]
    room = jnp.minimum(tallies[source_of] - 1, most - tallies[sink]) // 2
    room = jnp.where((source_of == ranking[0]) | (sink == ranking[0]) | (tallies[sink] == 0), 0, jnp.maximum(room, 0))
    moved = jax.random.randint(jax.random.fold_in(own, 4), (count // 2,), 0, 1 << 20) % (room + 1)
    tallies = tallies.at[source_of].add(-moved).at[sink].add(moved)
    members = jnp.searchsorted(jnp.cumsum(tallies), jnp.arange(rows * top), side="right").astype(jnp.int32)
    table = members.reshape(top, rows).T
    table = table[jax.random.permutation(jax.random.fold_in(own, 1), rows)]
    offset_by = jax.random.randint(jax.random.fold_in(own, 2), (rows, 1), 0, top)
    return jnp.take_along_axis(table, (jnp.arange(top)[None, :] + offset_by) % top, axis=1)


def shares(number_of, total, most, skew, full):
    portions = [(1 << 20) // math.isqrt(standing ** skew) + 1 for standing in range(1, number_of + 1)]
    largest = most if full else min(most, max(-(-total // number_of), total * portions[0] // sum(portions)))
    least = 1 if total - largest >= number_of - 1 else 0
    given, rest = [largest] + [least] * (number_of - 1), total - largest - least * (number_of - 1)
    while rest > 0:
        candidates = [i for i in range(1, number_of) if given[i] < largest] or [i for i in range(1, number_of) if given[i] < most]
        pool, left = sum([portions[i] for i in candidates]), rest
        for i in candidates:
            more = min(most - given[i], max(1, left * portions[i] // pool), rest)
            given[i] = given[i] + more
            rest = rest - more
    return np.array(given)


def scatter_about(own_key, extent, spread, bound, cuts=(), kind=jnp.bfloat16):
    result = spread * jax.random.normal(own_key, extent, jnp.float32)
    if cuts:
        result = result * block_scale(own_key, extent, cuts, -0.22, 0.18)
    return jnp.clip(result, -bound, bound).astype(kind)


def setup_inputs(seed: int = 0) -> dict:
    key_list = jax.random.split(jax.random.key(seed), 9)
    cotangents = scatter_about(key_list[0], (TOKENS, DW), 0.1, 0.59765625, ((0, 32),))
    routes_keys = jax.random.split(jax.random.fold_in(key_list[1], 1), TOKENS // TOK_DEV)
    routes_turns = jax.random.permutation(jax.random.fold_in(key_list[1], 3), TOKENS // TOK_DEV)
    routes = jax.vmap(lambda own, number: assign_block(jax.random.fold_in(key_list[1], 2), own, number, TOK_DEV, EXPERTS, 2, CAP, 2))(routes_keys, routes_turns).reshape((TOKENS, 2))
    gate_probs = jnp.clip(0.1 + 0.79999997 * jax.random.uniform(key_list[2], (TOKENS, 2), jnp.float32) ** block_scale(key_list[2], (TOKENS, 2), ((0, 32),), -0.2, 0.2), 0.1, 0.9)
    hidden_now = scatter_about(key_list[3], (EXPERTS, N_DP, EXPERTS, CAP, FFW), 1.0, 6.0, ((0, 4), (1, 8)))
    hidden_prev = scatter_about(key_list[4], (EXPERTS, N_DP, EXPERTS, CAP, FFW), 1.0, 6.0, ((0, 4), (1, 8)))
    cotan_prev = scatter_about(key_list[5], (EXPERTS, N_DP, EXPERTS * CAP, DW), 0.05, 0.29882812, ((0, 4), (1, 8)))
    trigger = draw_trigger(jax.random.fold_in(key_list[8], 71), 0)
    stale_sum = scatter_about(key_list[7], (EXPERTS, FFW, DW), 2.0, 12.0, ((0, 4), (2, 8)), jnp.float32)
    return dict(cotangents=cotangents, routes=routes, gate_probs=gate_probs, hidden_now=hidden_now, hidden_prev=hidden_prev, cotan_prev=cotan_prev, trigger=trigger, stale_sum=stale_sum)


trigger_weight = 0.1


def slot_rows(routes_dev, probs_dev, cotan_dev):
    flat_routes = routes_dev.reshape(-1).astype(jnp.int32)
    onehot = (flat_routes[:, None] == jnp.arange(EXPERTS, dtype=jnp.int32)[None, :]).astype(jnp.int32)
    slot_ranks = jnp.sum((jnp.cumsum(onehot, axis=0) - 1) * onehot, axis=1)
    target = (flat_routes * CAP + slot_ranks).astype(jnp.int32)
    weighted = jnp.repeat(cotan_dev.astype(jnp.float32), 2, axis=0) * probs_dev.reshape(-1)[:, None]
    send_table = jnp.zeros((EXPERTS * CAP, DW), jnp.float32).at[target].add(weighted)
    return send_table.astype(jnp.bfloat16).reshape(EXPERTS, CAP, DW)


def reference(cotangents, routes, gate_probs, hidden_now, hidden_prev, cotan_prev, trigger, stale_sum):
    devices_all = EXPERTS * N_DP
    slot_tables = jax.vmap(slot_rows)(routes.reshape(devices_all, TOK_DEV, 2), gate_probs.reshape(devices_all, TOK_DEV, 2), cotangents.reshape(devices_all, TOK_DEV, DW))
    slot_tables = slot_tables.reshape(EXPERTS, N_DP, EXPERTS, CAP, DW)

    def one_expert(expert):
        def one_worker(running_sum, worker):
            arrived = slot_tables[:, worker, expert]
            stacked_left = jnp.concatenate([hidden_now[expert, worker].reshape(-1, FFW), hidden_prev[expert, worker].reshape(-1, FFW)], axis=0).astype(jnp.float32)
            stacked_right = jnp.concatenate([arrived.reshape(-1, DW), -cotan_prev[expert, worker]], axis=0).astype(jnp.float32)
            difference = jnp.dot(stacked_left.T, stacked_right, precision=lax.Precision.HIGHEST)
            blocks = difference.reshape(BLOCKS, BLOCK, DW)
            diff_norms = jnp.mean(blocks * blocks, axis=(1, 2))
            gate_values = trigger[expert, worker].astype(jnp.float32)
            sent_terms = (blocks * gate_values[:, None, None]).astype(jnp.bfloat16)
            sent_terms = lax.optimization_barrier(sent_terms).astype(jnp.float32)
            return running_sum + sent_terms, diff_norms

        zero_start = jnp.zeros((BLOCKS, BLOCK, DW), jnp.float32)
        summed_terms, diff_norms = lax.scan(one_worker, zero_start, jnp.arange(N_DP))
        new_block = stale_sum[expert] + summed_terms.reshape(FFW, DW)
        block_means = jnp.sum((new_block * new_block).reshape(BLOCKS, BLOCK * DW), axis=1) / (BLOCK * DW)
        return new_block, diff_norms - trigger_weight * block_means[None, :]

    new_sum, margins = lax.map(one_expert, jnp.arange(EXPERTS))
    return new_sum, margins
```

```python
import functools

import jax
import jax.numpy as jnp
from jax import lax
from jax.experimental import pallas as pl
from jax.experimental.pallas import tpu as pltpu
from jax.sharding import PartitionSpec as P

BLOCK = 128
TRIG = 16
LANES = 128
trigger_weight = 0.1
MESH = pl.DeviceIdType.MESH
TN = (((0,), (0,)), ((), ()))


def params(**kw):
    return pltpu.CompilerParams(vmem_limit_bytes=60 * 1024 * 1024, **kw)


def greet(axis, n, me):
    barrier = pltpu.get_barrier_semaphore()
    for step in range(1, n):
        pl.semaphore_signal(
            barrier, inc=1, device_id={axis: lax.rem(me + step, n)}, device_id_type=MESH
        )
    pl.semaphore_wait(barrier, n - 1)


def table_kernel(n, capacity, routes_ref, gates_ref, cotan_ref, out_ref):
    tokens = cotan_ref.shape[0]
    experts = lax.broadcasted_iota(jnp.int32, (n, tokens), 0)
    first = routes_ref[0:1, :] == experts
    second = routes_ref[1:2, :] == experts
    named = jnp.where(first | second, 1.0, 0.0)
    gates = jnp.where(first, gates_ref[0:1, :], 0.0) + jnp.where(second, gates_ref[1:2, :], 0.0)
    earlier = jnp.where(
        lax.broadcasted_iota(jnp.int32, (tokens, tokens), 0)
        < lax.broadcasted_iota(jnp.int32, (tokens, tokens), 1),
        1.0,
        0.0,
    )
    ranks = jnp.dot(
        named.astype(jnp.bfloat16), earlier.astype(jnp.bfloat16), preferred_element_type=jnp.float32
    )
    ranks = jnp.where(named > 0.5, ranks, -1.0)
    slot = lax.broadcasted_iota(jnp.int32, (capacity, tokens), 0).astype(jnp.float32)
    for e in range(n):
        place = jnp.where(slot == ranks[e : e + 1, :], 1.0, 0.0)
        weight = jnp.sum(place * gates[e : e + 1, :], axis=1, keepdims=True)
        rows = jnp.dot(
            place.astype(jnp.bfloat16), cotan_ref[...], preferred_element_type=jnp.float32
        )
        out_ref[e] = (rows * weight).astype(jnp.bfloat16)


def exchange_kernel(n, table_ref, out_ref, own_sem, send_sem, recv_sem):
    me = lax.axis_index("expert")
    greet("expert", n, me)
    copies = []
    for step in range(1, n):
        peer = lax.rem(me + step, n)
        copy = pltpu.make_async_remote_copy(
            src_ref=table_ref.at[peer],
            dst_ref=out_ref.at[me],
            send_sem=send_sem.at[step],
            recv_sem=recv_sem.at[step],
            device_id={"expert": peer},
            device_id_type=MESH,
        )
        copy.start()
        copies.append(copy)
    own = pltpu.make_async_copy(table_ref.at[me], out_ref.at[me], own_sem)
    own.start()
    own.wait()
    for copy in copies:
        copy.wait()


def dispatch(routes, gates, cotangents, n, capacity):
    width = cotangents.shape[1]
    shape = jax.ShapeDtypeStruct((n, capacity, width), jnp.bfloat16)
    table = pl.pallas_call(
        functools.partial(table_kernel, n, capacity),
        out_shape=shape,
        compiler_params=params(),
        name="table",
    )(routes, gates, cotangents)
    return pl.pallas_call(
        functools.partial(exchange_kernel, n),
        out_shape=shape,
        in_specs=[pl.BlockSpec(memory_space=pltpu.VMEM)],
        out_specs=pl.BlockSpec(memory_space=pltpu.VMEM),
        scratch_shapes=[
            pltpu.SemaphoreType.DMA,
            pltpu.SemaphoreType.DMA((n,)),
            pltpu.SemaphoreType.DMA((n,)),
        ],
        compiler_params=params(collective_id=0, has_side_effects=True),
        name="exchange",
    )(table)


def picked_kernel(parts, picked_ref, now_ref, prev_ref, arrived_ref, cotan_ref, out_ref):
    columns = out_ref.shape[-1]
    per = 4 if parts % 4 == 0 else 1
    wide = columns * parts // per
    keep = jnp.where(picked_ref[1, pl.program_id(0)] > 0, 1.0, 0.0)
    for q in range(per):
        cut = slice(q * wide, (q + 1) * wide)
        total = lax.dot_general(
            now_ref[...], arrived_ref[:, cut], TN, preferred_element_type=jnp.float32
        ) - lax.dot_general(
            prev_ref[...], cotan_ref[:, cut], TN, preferred_element_type=jnp.float32
        )
        total = (total * keep).astype(jnp.bfloat16)
        for p in range(parts // per):
            out_ref[q * (parts // per) + p, 0] = total[:, p * columns : (p + 1) * columns]


def picked_blocks(picked, now, prev, arrived, cotan, parts):
    rows, width = arrived.shape
    columns = width // parts
    return pl.pallas_call(
        functools.partial(picked_kernel, parts),
        out_shape=jax.ShapeDtypeStruct((parts, TRIG, BLOCK, columns), jnp.bfloat16),
        grid_spec=pltpu.PrefetchScalarGridSpec(
            num_scalar_prefetch=1,
            grid=(TRIG,),
            in_specs=[
                pl.BlockSpec((rows, BLOCK), lambda k, ids: (0, ids[0, k])),
                pl.BlockSpec((rows, BLOCK), lambda k, ids: (0, ids[0, k])),
                pl.BlockSpec((rows, width), lambda k, ids: (0, 0)),
                pl.BlockSpec((rows, width), lambda k, ids: (0, 0)),
            ],
            out_specs=pl.BlockSpec((parts, 1, BLOCK, columns), lambda k, ids: (0, k, 0, 0)),
        ),
        compiler_params=params(dimension_semantics=("arbitrary",)),
        cost_estimate=pl.CostEstimate(
            flops=4 * TRIG * BLOCK * rows * width, bytes_accessed=4 * TRIG * BLOCK * width, transcendentals=0
        ),
        name="picked",
    )(picked, now, prev, arrived, cotan)


def norms_kernel(group, now_ref, prev_ref, arrived_ref, cotan_ref, out_ref):
    width = arrived_ref.shape[1]
    step = 512 if width % 512 == 0 else width
    sums = [jnp.zeros((1, LANES), jnp.float32) for _ in range(group)]
    for q in range(width // step):
        cut = slice(q * step, (q + 1) * step)
        total = lax.dot_general(
            now_ref[...], arrived_ref[:, cut], TN, preferred_element_type=jnp.float32
        ) - lax.dot_general(
            prev_ref[...], cotan_ref[:, cut], TN, preferred_element_type=jnp.float32
        )
        square = total * total
        for g in range(group):
            part = jnp.sum(square[g * BLOCK : (g + 1) * BLOCK], axis=0, keepdims=True)
            for i in range(step // LANES):
                sums[g] = sums[g] + part[:, i * LANES : (i + 1) * LANES]
    for g in range(group):
        out_ref[g] = sums[g]


def block_norms(now, prev, arrived, cotan):
    rows, width = arrived.shape
    blocks = now.shape[1] // BLOCK
    group = 4 if blocks % 4 == 0 else 1
    return pl.pallas_call(
        functools.partial(norms_kernel, group),
        out_shape=jax.ShapeDtypeStruct((blocks, 1, LANES), jnp.float32),
        grid=(blocks // group,),
        in_specs=[
            pl.BlockSpec((rows, group * BLOCK), lambda b: (0, b)),
            pl.BlockSpec((rows, group * BLOCK), lambda b: (0, b)),
            pl.BlockSpec((rows, width), lambda b: (0, 0)),
            pl.BlockSpec((rows, width), lambda b: (0, 0)),
        ],
        out_specs=pl.BlockSpec((group, 1, LANES), lambda b: (b, 0, 0)),
        compiler_params=params(dimension_semantics=("arbitrary",)),
        cost_estimate=pl.CostEstimate(
            flops=4 * now.shape[1] * rows * width, bytes_accessed=4 * now.size, transcendentals=0
        ),
        name="norms",
    )(now, prev, arrived, cotan)


def add_kernel(workers, table_ref, stale_ref, landed_ref, out_ref, square_ref):
    b = pl.program_id(0)
    out_ref[...] = stale_ref[...]
    for w in range(workers):
        index = table_ref[w, b]

        @pl.when(index >= 0)
        def _():
            out_ref[0] += landed_ref[w, index].astype(jnp.float32)

    new = out_ref[0]
    part = jnp.sum(new * new, axis=0, keepdims=True)
    total = part[:, 0:LANES]
    for i in range(1, new.shape[1] // LANES):
        total = total + part[:, i * LANES : (i + 1) * LANES]
    square_ref[0] = total


def add_landed(table, stale, landed):
    workers, slots, _, columns = landed.shape
    blocks = stale.shape[0]
    return pl.pallas_call(
        functools.partial(add_kernel, workers),
        out_shape=(
            jax.ShapeDtypeStruct(stale.shape, jnp.float32),
            jax.ShapeDtypeStruct((blocks, 1, LANES), jnp.float32),
        ),
        grid_spec=pltpu.PrefetchScalarGridSpec(
            num_scalar_prefetch=1,
            grid=(blocks,),
            in_specs=[
                pl.BlockSpec((1, BLOCK, columns), lambda b, ids: (b, 0, 0)),
                pl.BlockSpec((workers, slots, BLOCK, columns), lambda b, ids: (0, 0, 0, 0)),
            ],
            out_specs=(
                pl.BlockSpec((1, BLOCK, columns), lambda b, ids: (b, 0, 0)),
                pl.BlockSpec((1, 1, LANES), lambda b, ids: (b, 0, 0)),
            ),
        ),
        compiler_params=params(dimension_semantics=("arbitrary",)),
        cost_estimate=pl.CostEstimate(flops=4 * stale.size, bytes_accessed=10 * stale.size, transcendentals=0),
        name="addlanded",
    )(table, stale, landed)


def total_kernel(n, part_ref, out_ref, landed, send_sem, recv_sem):
    me = lax.axis_index("dp")
    greet("dp", n, me)
    copies = []
    for step in range(1, n):
        copy = pltpu.make_async_remote_copy(
            src_ref=part_ref,
            dst_ref=landed.at[step],
            send_sem=send_sem.at[step],
            recv_sem=recv_sem.at[step],
            device_id={"dp": lax.rem(me + step, n)},
            device_id_type=MESH,
        )
        copy.start()
        copies.append(copy)
    for copy in copies:
        copy.wait()
    total = part_ref[...]
    for step in range(1, n):
        total = total + landed[step]
    out_ref[...] = total


def shared_total(part, n):
    return pl.pallas_call(
        functools.partial(total_kernel, n),
        out_shape=jax.ShapeDtypeStruct(part.shape, jnp.float32),
        in_specs=[pl.BlockSpec(memory_space=pltpu.VMEM)],
        out_specs=pl.BlockSpec(memory_space=pltpu.VMEM),
        scratch_shapes=[
            pltpu.VMEM((n,) + part.shape, jnp.float32),
            pltpu.SemaphoreType.DMA((n,)),
            pltpu.SemaphoreType.DMA((n,)),
        ],
        compiler_params=params(collective_id=1, has_side_effects=True),
        name="total",
    )(part)


def local(cotangents, routes, gate_probs, hidden_now, hidden_prev, cotan_prev, trigger, stale_sum):
    experts = lax.axis_size("expert")
    workers = lax.axis_size("dp")
    capacity, ffw = hidden_now.shape[3:]
    width = cotangents.shape[1]
    columns = width // workers
    blocks = ffw // BLOCK
    now = hidden_now.reshape(-1, ffw)
    prev = hidden_prev.reshape(-1, ffw)
    cotan = cotan_prev.reshape(-1, width)

    row = trigger.reshape(-1)
    running = jnp.cumsum(row)
    order = jnp.arange(1, TRIG + 1, dtype=jnp.int32)[:, None]
    chosen = (row[None, :] == 1) & (running[None, :] == order)
    ids = jnp.sum(jnp.where(chosen, jnp.arange(blocks, dtype=jnp.int32)[None, :], 0), axis=1)
    filled = jnp.sum(chosen.astype(jnp.int32), axis=1)
    rows = lax.all_gather(row, "dp")
    table = jnp.where(rows == 1, jnp.cumsum(rows, axis=1) - 1, -1)

    arrived = dispatch(routes.T, gate_probs.T, cotangents, experts, capacity).reshape(-1, width)
    packed = picked_blocks(jnp.stack([ids, filled]), now, prev, arrived, cotan, workers)
    landed = lax.all_to_all(packed, "dp", split_axis=0, concat_axis=0, tiled=True)
    norms = block_norms(now, prev, arrived, cotan)
    new, squares = add_landed(table, stale_sum.reshape(blocks, BLOCK, columns), landed)
    totals = shared_total(squares.reshape(blocks, LANES), workers)
    margins = jnp.sum(norms.reshape(blocks, LANES) - trigger_weight * totals, axis=1) / (BLOCK * width)
    return new.reshape(1, ffw, columns), margins.reshape(1, 1, blocks)


def solution(mesh):
    return jax.shard_map(
        local,
        mesh=mesh,
        in_specs=(
            P(("expert", "dp"), None),
            P(("expert", "dp"), None),
            P(("expert", "dp"), None),
            P("expert", "dp", None, None, None),
            P("expert", "dp", None, None, None),
            P("expert", "dp", None, None),
            P("expert", "dp", None),
            P("expert", None, "dp"),
        ),
        out_specs=(P("expert", None, "dp"), P("expert", "dp", None)),
        check_vma=False,
    )
```

```python
import functools

import jax
import jax.numpy as jnp
from jax import lax
from jax.experimental import pallas as pl
from jax.experimental.pallas import tpu as pltpu
from jax.sharding import PartitionSpec as P

BLOCK = 128
TRIG = 16
LANES = 128
trigger_weight = 0.1
MESH = pl.DeviceIdType.MESH
TN = (((0,), (0,)), ((), ()))


def params(**kw):
    return pltpu.CompilerParams(vmem_limit_bytes=60 * 1024 * 1024, **kw)


def greet(axis, n, me):
    barrier = pltpu.get_barrier_semaphore()
    for step in range(1, n):
        pl.semaphore_signal(
            barrier, inc=1, device_id={axis: lax.rem(me + step, n)}, device_id_type=MESH
        )
    pl.semaphore_wait(barrier, n - 1)


def table_kernel(n, capacity, routes_ref, gates_ref, cotan_ref, out_ref):
    tokens = cotan_ref.shape[0]
    experts = lax.broadcasted_iota(jnp.int32, (n, tokens), 0)
    first = routes_ref[0:1, :] == experts
    second = routes_ref[1:2, :] == experts
    named = jnp.where(first | second, 1.0, 0.0)
    gates = jnp.where(first, gates_ref[0:1, :], 0.0) + jnp.where(second, gates_ref[1:2, :], 0.0)
    earlier = jnp.where(
        lax.broadcasted_iota(jnp.int32, (tokens, tokens), 0)
        < lax.broadcasted_iota(jnp.int32, (tokens, tokens), 1),
        1.0,
        0.0,
    )
    ranks = jnp.dot(
        named.astype(jnp.bfloat16), earlier.astype(jnp.bfloat16), preferred_element_type=jnp.float32
    )
    ranks = jnp.where(named > 0.5, ranks, -1.0)
    slot = lax.broadcasted_iota(jnp.int32, (capacity, tokens), 0).astype(jnp.float32)
    for e in range(n):
        place = jnp.where(slot == ranks[e : e + 1, :], 1.0, 0.0)
        weight = jnp.sum(place * gates[e : e + 1, :], axis=1, keepdims=True)
        rows = jnp.dot(
            place.astype(jnp.bfloat16), cotan_ref[...], preferred_element_type=jnp.float32
        )
        out_ref[e] = (rows * weight).astype(jnp.bfloat16)


def exchange_kernel(n, table_ref, out_ref, own_sem, send_sem, recv_sem):
    me = lax.axis_index("expert")
    greet("expert", n, me)
    copies = []
    for step in range(1, n):
        peer = lax.rem(me + step, n)
        copy = pltpu.make_async_remote_copy(
            src_ref=table_ref.at[peer],
            dst_ref=out_ref.at[me],
            send_sem=send_sem.at[step],
            recv_sem=recv_sem.at[step],
            device_id={"expert": peer},
            device_id_type=MESH,
        )
        copy.start()
        copies.append(copy)
    own = pltpu.make_async_copy(table_ref.at[me], out_ref.at[me], own_sem)
    own.start()
    own.wait()
    for copy in copies:
        copy.wait()


def dispatch(routes, gates, cotangents, n, capacity):
    width = cotangents.shape[1]
    shape = jax.ShapeDtypeStruct((n, capacity, width), jnp.bfloat16)
    table = pl.pallas_call(
        functools.partial(table_kernel, n, capacity),
        out_shape=shape,
        compiler_params=params(),
        name="table",
    )(routes, gates, cotangents)
    return pl.pallas_call(
        functools.partial(exchange_kernel, n),
        out_shape=shape,
        in_specs=[pl.BlockSpec(memory_space=pltpu.VMEM)],
        out_specs=pl.BlockSpec(memory_space=pltpu.VMEM),
        scratch_shapes=[
            pltpu.SemaphoreType.DMA,
            pltpu.SemaphoreType.DMA((n,)),
            pltpu.SemaphoreType.DMA((n,)),
        ],
        compiler_params=params(collective_id=0, has_side_effects=True),
        name="exchange",
    )(table)


def picked_kernel(parts, picked_ref, now_ref, prev_ref, arrived_ref, cotan_ref, out_ref):
    columns = out_ref.shape[-1]
    per = 4 if parts % 4 == 0 else 1
    wide = columns * parts // per
    keep = jnp.where(picked_ref[1, pl.program_id(0)] > 0, 1.0, 0.0)
    for q in range(per):
        cut = slice(q * wide, (q + 1) * wide)
        total = lax.dot_general(
            now_ref[...], arrived_ref[:, cut], TN, preferred_element_type=jnp.float32
        ) - lax.dot_general(
            prev_ref[...], cotan_ref[:, cut], TN, preferred_element_type=jnp.float32
        )
        total = (total * keep).astype(jnp.bfloat16)
        for p in range(parts // per):
            out_ref[q * (parts // per) + p, 0] = total[:, p * columns : (p + 1) * columns]


def picked_blocks(picked, now, prev, arrived, cotan, parts):
    rows, width = arrived.shape
    columns = width // parts
    return pl.pallas_call(
        functools.partial(picked_kernel, parts),
        out_shape=jax.ShapeDtypeStruct((parts, TRIG, BLOCK, columns), jnp.bfloat16),
        grid_spec=pltpu.PrefetchScalarGridSpec(
            num_scalar_prefetch=1,
            grid=(TRIG,),
            in_specs=[
                pl.BlockSpec((rows, BLOCK), lambda k, ids: (0, ids[0, k])),
                pl.BlockSpec((rows, BLOCK), lambda k, ids: (0, ids[0, k])),
                pl.BlockSpec((rows, width), lambda k, ids: (0, 0)),
                pl.BlockSpec((rows, width), lambda k, ids: (0, 0)),
            ],
            out_specs=pl.BlockSpec((parts, 1, BLOCK, columns), lambda k, ids: (0, k, 0, 0)),
        ),
        compiler_params=params(dimension_semantics=("arbitrary",)),
        cost_estimate=pl.CostEstimate(
            flops=4 * TRIG * BLOCK * rows * width, bytes_accessed=4 * TRIG * BLOCK * width, transcendentals=0
        ),
        name="picked",
    )(picked, now, prev, arrived, cotan)


def norms_kernel(group, now_ref, prev_ref, arrived_ref, cotan_ref, out_ref):
    width = arrived_ref.shape[1]
    step = 512 if width % 512 == 0 else width
    sums = [jnp.zeros((1, LANES), jnp.float32) for _ in range(group)]
    for q in range(width // step):
        cut = slice(q * step, (q + 1) * step)
        total = lax.dot_general(
            now_ref[...], arrived_ref[:, cut], TN, preferred_element_type=jnp.float32
        ) - lax.dot_general(
            prev_ref[...], cotan_ref[:, cut], TN, preferred_element_type=jnp.float32
        )
        square = total * total
        for g in range(group):
            part = jnp.sum(square[g * BLOCK : (g + 1) * BLOCK], axis=0, keepdims=True)
            for i in range(step // LANES):
                sums[g] = sums[g] + part[:, i * LANES : (i + 1) * LANES]
    for g in range(group):
        out_ref[g] = sums[g]


def block_norms(now, prev, arrived, cotan):
    rows, width = arrived.shape
    blocks = now.shape[1] // BLOCK
    group = 4 if blocks % 4 == 0 else 1
    return pl.pallas_call(
        functools.partial(norms_kernel, group),
        out_shape=jax.ShapeDtypeStruct((blocks, 1, LANES), jnp.float32),
        grid=(blocks // group,),
        in_specs=[
            pl.BlockSpec((rows, group * BLOCK), lambda b: (0, b)),
            pl.BlockSpec((rows, group * BLOCK), lambda b: (0, b)),
            pl.BlockSpec((rows, width), lambda b: (0, 0)),
            pl.BlockSpec((rows, width), lambda b: (0, 0)),
        ],
        out_specs=pl.BlockSpec((group, 1, LANES), lambda b: (b, 0, 0)),
        compiler_params=params(dimension_semantics=("arbitrary",)),
        cost_estimate=pl.CostEstimate(
            flops=4 * now.shape[1] * rows * width, bytes_accessed=4 * now.size, transcendentals=0
        ),
        name="norms",
    )(now, prev, arrived, cotan)


def add_kernel(workers, group, table_ref, stale_ref, landed_ref, out_ref, square_ref):
    out_ref[...] = stale_ref[...]
    for g in range(group):
        b = pl.program_id(0) * group + g
        for w in range(workers):
            index = table_ref[w, b]

            @pl.when(index >= 0)
            def _():
                out_ref[g] += landed_ref[w, index].astype(jnp.float32)

        new = out_ref[g]
        part = jnp.sum(new * new, axis=0, keepdims=True)
        total = part[:, 0:LANES]
        for i in range(1, new.shape[1] // LANES):
            total = total + part[:, i * LANES : (i + 1) * LANES]
        square_ref[g] = total


def add_landed(table, stale, landed):
    workers, slots, _, columns = landed.shape
    blocks = stale.shape[0]
    group = 4 if blocks % 4 == 0 else 1
    return pl.pallas_call(
        functools.partial(add_kernel, workers, group),
        out_shape=(
            jax.ShapeDtypeStruct(stale.shape, jnp.float32),
            jax.ShapeDtypeStruct((blocks, 1, LANES), jnp.float32),
        ),
        grid_spec=pltpu.PrefetchScalarGridSpec(
            num_scalar_prefetch=1,
            grid=(blocks // group,),
            in_specs=[
                pl.BlockSpec((group, BLOCK, columns), lambda b, ids: (b, 0, 0)),
                pl.BlockSpec((workers, slots, BLOCK, columns), lambda b, ids: (0, 0, 0, 0)),
            ],
            out_specs=(
                pl.BlockSpec((group, BLOCK, columns), lambda b, ids: (b, 0, 0)),
                pl.BlockSpec((group, 1, LANES), lambda b, ids: (b, 0, 0)),
            ),
        ),
        compiler_params=params(dimension_semantics=("arbitrary",)),
        cost_estimate=pl.CostEstimate(flops=4 * stale.size, bytes_accessed=10 * stale.size, transcendentals=0),
        name="addlanded",
    )(table, stale, landed)


def total_kernel(n, part_ref, out_ref, landed, send_sem, recv_sem):
    me = lax.axis_index("dp")
    greet("dp", n, me)
    copies = []
    for step in range(1, n):
        copy = pltpu.make_async_remote_copy(
            src_ref=part_ref,
            dst_ref=landed.at[step],
            send_sem=send_sem.at[step],
            recv_sem=recv_sem.at[step],
            device_id={"dp": lax.rem(me + step, n)},
            device_id_type=MESH,
        )
        copy.start()
        copies.append(copy)
    for copy in copies:
        copy.wait()
    total = part_ref[...]
    for step in range(1, n):
        total = total + landed[step]
    out_ref[...] = total


def shared_total(part, n):
    return pl.pallas_call(
        functools.partial(total_kernel, n),
        out_shape=jax.ShapeDtypeStruct(part.shape, jnp.float32),
        in_specs=[pl.BlockSpec(memory_space=pltpu.VMEM)],
        out_specs=pl.BlockSpec(memory_space=pltpu.VMEM),
        scratch_shapes=[
            pltpu.VMEM((n,) + part.shape, jnp.float32),
            pltpu.SemaphoreType.DMA((n,)),
            pltpu.SemaphoreType.DMA((n,)),
        ],
        compiler_params=params(collective_id=1, has_side_effects=True),
        name="total",
    )(part)


def local(cotangents, routes, gate_probs, hidden_now, hidden_prev, cotan_prev, trigger, stale_sum):
    experts = lax.axis_size("expert")
    workers = lax.axis_size("dp")
    capacity, ffw = hidden_now.shape[3:]
    width = cotangents.shape[1]
    columns = width // workers
    blocks = ffw // BLOCK
    now = hidden_now.reshape(-1, ffw)
    prev = hidden_prev.reshape(-1, ffw)
    cotan = cotan_prev.reshape(-1, width)

    row = trigger.reshape(-1)
    running = jnp.cumsum(row)
    order = jnp.arange(1, TRIG + 1, dtype=jnp.int32)[:, None]
    chosen = (row[None, :] == 1) & (running[None, :] == order)
    ids = jnp.sum(jnp.where(chosen, jnp.arange(blocks, dtype=jnp.int32)[None, :], 0), axis=1)
    filled = jnp.sum(chosen.astype(jnp.int32), axis=1)
    rows = lax.all_gather(row, "dp")
    rows, routes, gate_probs = lax.optimization_barrier((rows, routes, gate_probs))
    table = jnp.where(rows == 1, jnp.cumsum(rows, axis=1) - 1, -1)

    arrived = dispatch(routes.T, gate_probs.T, cotangents, experts, capacity).reshape(-1, width)
    packed = picked_blocks(jnp.stack([ids, filled]), now, prev, arrived, cotan, workers)
    landed = lax.all_to_all(packed, "dp", split_axis=0, concat_axis=0, tiled=True)
    norms = block_norms(now, prev, arrived, cotan)
    new, squares = add_landed(table, stale_sum.reshape(blocks, BLOCK, columns), landed)
    totals = shared_total(squares.reshape(blocks, LANES), workers)
    margins = jnp.sum(norms.reshape(blocks, LANES) - trigger_weight * totals, axis=1) / (BLOCK * width)
    return new.reshape(1, ffw, columns), margins.reshape(1, 1, blocks)


def solution(mesh):
    return jax.shard_map(
        local,
        mesh=mesh,
        in_specs=(
            P(("expert", "dp"), None),
            P(("expert", "dp"), None),
            P(("expert", "dp"), None),
            P("expert", "dp", None, None, None),
            P("expert", "dp", None, None, None),
            P("expert", "dp", None, None),
            P("expert", "dp", None),
            P("expert", None, "dp"),
        ),
        out_specs=(P("expert", None, "dp"), P("expert", "dp", None)),
        check_vma=False,
    )
```
